64 devices in a mesh: dp: 8 (over x, y, core), tp: 8 (over z).
Axes of the slice: x: 2, y: 2, z: 8, core: 2. Of those that a mesh axis runs over, the one named last changes fastest.
The devices are a block of a 4x4x8 slice.
Arguments:
- x: bfloat16 [512, 8192], P('dp'), parts along dimension 0
- k_cache: bfloat16 [512, 2048, 8, 128], P('dp', None, 'tp'), parts along dimension 0
- v_cache: bfloat16 [512, 2048, 8, 128], P('dp', None, 'tp'), parts along dimension 0
- gain_a: bfloat16 [8192], replicated
- wq: bfloat16 [8192, 8192], P(None, 'tp')
- wo: bfloat16 [8192, 8192], P('tp')
- gain_m: bfloat16 [8192], replicated
- w_gate: bfloat16 [8192, 28672], P(None, 'tp')
- w_up: bfloat16 [8192, 28672], P(None, 'tp')
- w_down: bfloat16 [28672, 8192], P('tp')
Outputs:
- output: bfloat16 [512, 8192], P('dp'), parts along dimension 0
There are 8 independent parts. The reference program is written for one: setup_inputs(seed, part) draws one part's arguments, and reference() takes and returns one part's arrays. A program takes and returns all parts, laid end to end along the dimension named above; an argument that names none is the same for every part.
All inputs are finite; a program needn't handle non-finite values.
Results may differ from the reference program's by a relative error of at most 0.017.
Values are sent between devices in bfloat16 or wider.
A program may use at most 768 MiB of HBM per device.

```python
import jax
import jax.numpy as jnp
from jax import lax

BATCH = 64
CACHE = 2048
D = 8192
HEADS = 64
KV_HEADS = 8
HEAD = 128
FF = 28672
THETA = 10000


def setup_inputs(seed: int = 0, part: int = 0) -> dict:
    kx, kc, kw, kn, kq, ko, km, kg, ku, kd = jax.random.split(jax.random.key(seed), 10)
    kx, kc, kw = (jax.random.fold_in(k, part) for k in (kx, kc, kw))

    def weights(key, rows, columns):
        return jax.random.normal(key, (rows, columns), jnp.float32) * rows**-0.5

    drawn = {
        "x": jax.random.normal(kx, (BATCH, D), jnp.float32),
        "k_cache": 2 * jax.random.normal(kc, (BATCH, CACHE, KV_HEADS, HEAD), jnp.float32),
        "v_cache": 4 * jax.random.normal(kw, (BATCH, CACHE, KV_HEADS, HEAD), jnp.float32),
        "gain_a": 1 + 0.1 * jax.random.normal(kn, (D,), jnp.float32),
        "wq": 2 * weights(kq, D, HEADS * HEAD),
        "wo": weights(ko, HEADS * HEAD, D),
        "gain_m": 1 + 0.1 * jax.random.normal(km, (D,), jnp.float32),
        "w_gate": weights(kg, D, FF),
        "w_up": weights(ku, D, FF),
        "w_down": 2 * weights(kd, FF, D),
    }
    return {k: v.astype(jnp.bfloat16) for k, v in drawn.items()}


def normed(x, gain):
    wide = x.astype(jnp.float32)
    scale = lax.rsqrt(jnp.mean(wide * wide, -1, keepdims=True) + 1e-6)
    return (wide * scale * gain.astype(jnp.float32)).astype(jnp.bfloat16)


def turned(t, place, theta):
    half = t.shape[-1] // 2
    angle = place.astype(jnp.float32)[:, None] * theta ** (-jnp.arange(half, dtype=jnp.float32) / half)
    cos, sin = jnp.cos(angle)[:, None], jnp.sin(angle)[:, None]
    a, b = t[..., :half].astype(jnp.float32), t[..., half:].astype(jnp.float32)
    return jnp.concatenate([a * cos - b * sin, b * cos + a * sin], -1).astype(jnp.bfloat16)


def matmul(a, w):
    return jnp.dot(a, w, preferred_element_type=jnp.float32).astype(jnp.bfloat16)


def einsum(form, a, b):
    return jnp.einsum(form, a.astype(jnp.float32), b.astype(jnp.float32))


def seen_by(a, wq, k_cache, v_cache, head, theta):
    batch, cache, kv_heads = k_cache.shape[:3]
    place = jnp.full((batch,), cache - 1)
    q = turned(matmul(a, wq).reshape(batch, -1, head), place, theta).reshape(batch, kv_heads, -1, head)
    scores = einsum("bgsd,bugd->bgsu", q, k_cache) * head**-0.5
    weights = jax.nn.softmax(scores, -1).astype(jnp.bfloat16)
    return einsum("bgsu,bugd->bgsd", weights, v_cache).astype(jnp.bfloat16).reshape(batch, -1)


def hidden_of(b, w_gate, w_up):
    gate = jnp.dot(b, w_gate, preferred_element_type=jnp.float32)
    up = jnp.dot(b, w_up, preferred_element_type=jnp.float32)
    return (jax.nn.silu(gate) * up).astype(jnp.bfloat16)


def reference(x, k_cache, v_cache, gain_a, wq, wo, gain_m, w_gate, w_up, w_down):
    seen = seen_by(normed(x, gain_a), wq, k_cache, v_cache, HEAD, THETA)
    h = (x.astype(jnp.float32) + jnp.dot(seen, wo, preferred_element_type=jnp.float32)).astype(jnp.bfloat16)
    hidden = hidden_of(normed(h, gain_m), w_gate, w_up)
    return (h.astype(jnp.float32) + jnp.dot(hidden, w_down, preferred_element_type=jnp.float32)).astype(jnp.bfloat16)
```

```python
import functools

import jax
import jax.numpy as jnp
from jax import lax
from jax.experimental import pallas as pl
from jax.experimental.pallas import tpu as pltpu
from jax.sharding import PartitionSpec as P

HEAD = 128
THETA = 10000
F32, BF16 = jnp.float32, jnp.bfloat16

DEEP, WIDE = 4096, 256
SLOTS = 24
HELD = 8


def mult(v, k):
    return pl.multiple_of(v, k)


def layer(n, x_hbm, kc, vc, gain_a, wq, wo, gain_m, wg, wu, wd, cos, sin, out,
          ring, x, ab, states, part, hidden, q3, seen3, far1, near1, far2, near2, sf1, sn1, sf2, sn2,
          slot_sem, x_sem, send1, send2, rf1, rn1, rf2, rn2, gf1, gn1, gf2, gn2):
    me = lax.axis_index("tp")
    rows, d = x_hbm.shape
    head = kc.shape[2]
    keys = kc.shape[1]
    half = n // 2
    up_blocks = wg.shape[1] // WIDE
    down_rows = wd.shape[0]
    down_blocks = d // WIDE
    mlp = 4 * up_blocks + down_blocks
    chunk_rows = 16
    chunks = rows // chunk_rows

    def put(src, dst, slot):
        pltpu.make_async_copy(src, dst, slot_sem.at[slot]).start()

    def ready(slot, deep=DEEP):
        pltpu.make_async_copy(wg.at[pl.ds(0, deep), pl.ds(0, WIDE)], ring.at[slot, pl.ds(0, deep)], slot_sem.at[slot]).wait()

    def start_wq(cb, part_):
        slot = 2 * cb + part_
        put(wq.at[pl.ds(part_ * DEEP, DEEP), pl.ds(mult(cb * WIDE, WIDE), WIDE)], ring.at[slot], slot)

    def start_wo(cb):
        slot = HELD + cb
        for j in range(4):
            put(wo.at[:, pl.ds(mult(cb * 4 * WIDE + j * WIDE, WIDE), WIDE)], ring.at[slot, pl.ds(j * 1024, 1024)], slot)

    def kv_slot(j):
        return lax.rem(2 * HELD + lax.rem(j, SLOTS - HELD), SLOTS)

    def start_kv(it):
        for which, src in enumerate((kc, vc)):
            slot = kv_slot(2 * it + which)
            for p in range(2):
                for side in range(2):
                    put(src.at[it * 4 + 2 * p + side], ring.at[slot, pl.ds(p * keys, keys), pl.ds(side * head, head)], slot)

    def mlp_slot(m):
        return lax.rem(2 * HELD + m, SLOTS)

    def start_mlp4(m):
        @pl.when(m < 4 * up_blocks)
        def _():
            col = pl.ds(mult(m // 4 * WIDE, WIDE), WIDE)
            for r in range(4):
                slot = mlp_slot(m + r)
                put((wg, wu)[r // 2].at[pl.ds(r % 2 * DEEP, DEEP), col], ring.at[slot], slot)

        @pl.when((m >= 4 * up_blocks) & (m < mlp))
        def _():
            for r in range(4):
                slot = mlp_slot(m + r)
                nb = m + r - 4 * up_blocks
                put(wd.at[:, pl.ds(mult(nb * WIDE, WIDE), WIDE)], ring.at[slot, pl.ds(0, down_rows)], slot)

    x_copy = pltpu.make_async_copy(x_hbm, x, x_sem)
    x_copy.start()
    for cb in range(4):
        for part_ in range(2):
            start_wq(cb, part_)
    for it in range(4):
        start_kv(it)
    barrier = pltpu.get_barrier_semaphore()
    for step in (1, n - 1):
        pl.semaphore_signal(barrier, inc=1, device_id={"tp": lax.rem(me + step, n)}, device_id_type=pl.DeviceIdType.MESH)

    def steps(s, g, piece_rows, far, near, sf, sn, send, rf, rn, gf, gn, whole, residual, done):
        sign = 1 - 2 * lax.rem(g, 2)
        to_far = lax.rem(me + sign + n, n)
        to_near = lax.rem(me - sign + n, n)

        def owner(k):
            return lax.rem(me + k * sign + 2 * n, n)

        def at(o):
            return pl.ds(mult((g * n + o) * piece_rows, piece_rows), piece_rows)

        def remote(src, dst, i, sem, to):
            return pltpu.make_async_remote_copy(src_ref=src, dst_ref=dst, send_sem=send.at[i], recv_sem=sem,
                                                device_id={"tp": to}, device_id_type=pl.DeviceIdType.MESH)

        def far_copy(k):
            return remote(sf.at[k], far.at[g, k], k, rf.at[g, k], to_far)

        def near_copy(k):
            return remote(sn.at[k], near.at[g, k], half + k, rn.at[g, k], to_near)

        def far_out(k):
            piece = whole.at[at(owner(-k))]
            return remote(piece, piece, 2 * half - 1 + k, gf.at[g, k], to_far)

        def near_out(k):
            piece = whole.at[at(owner(k))]
            return remote(piece, piece, 3 * half - 1 + k, gn.at[g, k], to_near)

        def far_in(k):
            piece = whole.at[at(owner(-k - 1))]
            return remote(piece, piece, 2 * half - 1 + k, gf.at[g, k], to_far)

        def near_in(k):
            piece = whole.at[at(owner(k + 1))]
            return remote(piece, piece, 3 * half - 1 + k, gn.at[g, k], to_near)

        def free(copy):
            @pl.when(g > 0)
            def _():
                copy.wait_send()

        if s == "drain":
            for k in range(half):
                far_copy(k).wait_send()
                far_out(k).wait_send()
            for k in range(half - 1):
                near_copy(k).wait_send()
                near_out(k).wait_send()
            return
        if s < half:
            value = part[at(owner(half - s)), :]
            if s > 0:
                far_copy(s - 1).wait_recv()
                value = value + far[g, s - 1].astype(F32)
            free(far_copy(s))
            sf[s] = value.astype(BF16)
            far_copy(s).start()
        if 1 <= s < half:
            value = part[at(owner(s - half)), :]
            if s > 1:
                near_copy(s - 2).wait_recv()
                value = value + near[g, s - 2].astype(F32)
            free(near_copy(s - 1))
            sn[s - 1] = value.astype(BF16)
            near_copy(s - 1).start()
        if s == half:
            far_copy(half - 1).wait_recv()
            near_copy(half - 2).wait_recv()
            value = part[at(me), :] + far[g, half - 1].astype(F32) + near[g, half - 2].astype(F32)
            whole[at(me), :] = (residual(g) + value).astype(BF16)
            free(far_out(0))
            far_out(0).start()
            free(near_out(0))
            near_out(0).start()
        if half < s <= 2 * half:
            k = s - half - 1
            far_in(k).wait_recv()
            if k + 1 < half:
                free(far_out(k + 1))
                far_out(k + 1).start()
            if k < half - 1:
                near_in(k).wait_recv()
                if k + 1 < half - 1:
                    free(near_out(k + 1))
                    near_out(k + 1).start()
            if s == 2 * half:
                done(g)

    blocks = d // 128

    def norm_x(i, _):
        r = pl.ds(mult(i * 16, 16), 16)
        total = jnp.zeros((16, 128), F32)
        for k in range(blocks):
            wide = x[r, pl.ds(k * 128, 128)].astype(F32)
            total = total + wide * wide
        scale = lax.rsqrt(jnp.sum(total, -1, keepdims=True) * (1.0 / d) + 1e-6)
        for k in range(blocks):
            c = pl.ds(k * 128, 128)
            ab[r, c] = (x[r, c].astype(F32) * scale * gain_a[:, c]).astype(BF16)
        return 0

    x_copy.wait()
    lax.fori_loop(0, rows // 16, norm_x, 0)

    def project(cb, _):
        ready(2 * cb)
        acc = jnp.dot(ab[:, pl.ds(0, DEEP)], ring[2 * cb], preferred_element_type=F32)
        ready(2 * cb + 1)
        acc = acc + jnp.dot(ab[:, pl.ds(DEEP, DEEP)], ring[2 * cb + 1], preferred_element_type=F32)
        for j in range(2):
            t = acc[:, j * head:(j + 1) * head].astype(BF16).astype(F32)
            t = t * cos[...] + pltpu.roll(t, head // 2, 1) * sin[...]
            q3[pl.ds(2 * cb + j, rows, stride=8), :] = t.astype(BF16).astype(F32)
        start_kv(4 + cb)
        start_wo(2 * cb)
        start_wo(2 * cb + 1)
        return 0

    lax.fori_loop(0, 4, project, 0)
    pl.semaphore_wait(barrier, 2)

    def residual1(g):
        r = pl.ds(mult(g * chunk_rows, chunk_rows), chunk_rows)
        cols = [x[r, pl.ds(mult(me * 1024 + k * 128, 128), 128)].astype(F32) for k in range(8)]
        return jnp.concatenate(cols, 0)

    def done1(g):
        total = jnp.zeros((chunk_rows, 128), F32)
        for k in range(blocks):
            wide = states[pl.ds(mult(g * 1024 + k * 16, 16), 16), :].astype(F32)
            total = total + wide * wide
        scale = lax.rsqrt(jnp.sum(total, -1, keepdims=True) * (1.0 / d) + 1e-6)
        r = pl.ds(mult(g * chunk_rows, chunk_rows), chunk_rows)
        for k in range(blocks):
            c = pl.ds(k * 128, 128)
            wide = states[pl.ds(mult(g * 1024 + k * 16, 16), 16), :].astype(F32)
            ab[r, c] = (wide * scale * gain_m[:, c]).astype(BF16)

    first = functools.partial(steps, piece_rows=chunk_rows * 8, far=far1, near=near1, sf=sf1, sn=sn1,
                              send=send1, rf=rf1, rn=rn1, gf=gf1, gn=gn1, whole=states, residual=residual1, done=done1)

    def tick1(t):
        for s in range(2 * half, -1, -1):
            @pl.when((lax.rem(t - s + 16, 2) == 0) & (t >= s) & (t - s < 2 * chunks))
            def _():
                first(s, (t - s) // 2)

    def attend(it):
        ks, vs = kv_slot(2 * it), kv_slot(2 * it + 1)
        ready(ks)
        zero = jnp.zeros((8, head), F32)
        weights = []
        for p in range(2):
            s0 = (it * 4 + 2 * p) * 8
            q = jnp.concatenate([jnp.concatenate([q3[pl.ds(mult(s0, 8), 8), :], zero], 1),
                                 jnp.concatenate([zero, q3[pl.ds(mult(s0 + 8, 8), 8), :]], 1)], 0).astype(BF16)
            scores = lax.dot_general(q, ring[ks, pl.ds(p * keys, keys)], (((1,), (1,)), ((), ())),
                                     preferred_element_type=F32) * head**-0.5
            e = jnp.exp(scores - jnp.max(scores, -1, keepdims=True))
            weights.append((e * (1.0 / jnp.sum(e, -1, keepdims=True))).astype(BF16))
        ready(vs)
        for p in range(2):
            s0 = (it * 4 + 2 * p) * 8
            o = jnp.dot(weights[p], ring[vs, pl.ds(p * keys, keys)], preferred_element_type=F32)
            o = o.astype(BF16).astype(F32)
            seen3[pl.ds(mult(s0, 8), 8), :] = o[:8, :head]
            seen3[pl.ds(mult(s0 + 8, 8), 8), :] = o[8:, head:]

        @pl.when(it < 8)
        def _():
            start_kv(it + 8)

    def rows_chunk(c, _):
        def four(i, _):
            it = c * 4 + i
            attend(it)

            @pl.when((lax.rem(it, 2) == 1) & (it >= 8))
            def _():
                start_mlp4(2 * (it - 1 - 8))

            @pl.when(i == 1)
            def _():
                tick1(2 * c - 1)
            return 0

        lax.fori_loop(0, 4, four, 0)
        seen = jnp.concatenate([seen3[pl.ds(c * 128 + h, chunk_rows, stride=8), :] for h in range(8)], 1).astype(BF16)

        def columns(cb, _):
            @pl.when(c == 0)
            def _():
                ready(HELD + cb)
            for j in range(4):
                acc = jnp.dot(seen, ring[HELD + cb, pl.ds(j * 1024, 1024)], preferred_element_type=F32)
                base = (c * 8 + cb) * 128 + j * 32
                part[pl.ds(mult(base, 16), 16), :] = acc[:, :128]
                part[pl.ds(mult(base + 16, 16), 16), :] = acc[:, 128:]
            return 0

        lax.fori_loop(0, 8, columns, 0)
        tick1(2 * c)
        return 0

    lax.fori_loop(0, chunks, rows_chunk, 0)
    start_mlp4(16)
    start_mlp4(20)

    def rest1(t, _):
        tick1(t)
        return 0

    lax.fori_loop(2 * chunks - 1, 2 * (chunks - 1) + 2 * half + 1, rest1, 0)

    def gate_up(cb, _):
        m = 4 * cb
        outs = []
        for r in range(2):
            s0, s1 = mlp_slot(m + 2 * r), mlp_slot(m + 2 * r + 1)
            ready(s0)
            acc = jnp.dot(ab[:, pl.ds(0, DEEP)], ring[s0], preferred_element_type=F32)
            ready(s1)
            outs.append(acc + jnp.dot(ab[:, pl.ds(DEEP, DEEP)], ring[s1], preferred_element_type=F32))
        hidden[:, pl.ds(mult(cb * WIDE, WIDE), WIDE)] = (jax.nn.silu(outs[0]) * outs[1]).astype(BF16)
        start_mlp4(m + SLOTS)
        return 0

    lax.fori_loop(0, up_blocks, gate_up, 0)

    def residual2(g):
        pieces = [states[pl.ds(mult(c * 1024 + g * 128 + me * 16, 16), 16), :] for c in range(chunks)]
        return jnp.concatenate(pieces, 0).astype(F32)

    groups = d // 1024
    second = functools.partial(steps, piece_rows=rows, far=far2, near=near2, sf=sf2, sn=sn2,
                               send=send2, rf=rf2, rn=rn2, gf=gf2, gn=gn2, whole=out, residual=residual2, done=lambda g: None)

    def down(t, _):
        @pl.when(t < groups)
        def _():
            def block(i, _):
                nb = 4 * t + i
                slot = mlp_slot(4 * up_blocks + nb)
                ready(slot, down_rows)
                acc = jnp.dot(hidden[...], ring[slot, pl.ds(0, down_rows)], preferred_element_type=F32)
                part[pl.ds(mult(nb * 2 * rows, rows), rows), :] = acc[:, :128]
                part[pl.ds(mult(nb * 2 * rows + rows, rows), rows), :] = acc[:, 128:]
                return 0

            lax.fori_loop(0, 4, block, 0)
            start_mlp4(4 * up_blocks + 4 * t + SLOTS)

        for s in [0] + list(range(2 * half, 0, -1)):
            @pl.when((t >= s) & (t - s < groups))
            def _():
                second(s, t - s)
        return 0

    lax.fori_loop(0, groups + 2 * half, down, 0)
    first("drain", jnp.int32(chunks - 1))
    second("drain", jnp.int32(groups - 1))


def solution(mesh):
    n = mesh.shape["tp"]

    def step(x, k_cache, v_cache, gain_a, wq, wo, gain_m, w_gate, w_up, w_down):
        rows, d = x.shape
        batch, keys, _, head = k_cache.shape
        ff = w_gate.shape[1]
        place = jnp.full((1,), keys - 1)
        half = head // 2
        angle = place.astype(F32)[:, None] * THETA ** (-jnp.arange(half, dtype=F32) / half)
        cos, sin = jnp.cos(angle), jnp.sin(angle)
        cos = jnp.concatenate([cos, cos], -1)
        sin = jnp.concatenate([-sin, sin], -1)
        any_, vmem = pl.BlockSpec(memory_space=pl.ANY), pl.BlockSpec(memory_space=pltpu.VMEM)
        far, near = n // 2, n // 2 - 1
        chunks, groups = rows // 16, d // 1024
        dma = pltpu.SemaphoreType.DMA
        out = pl.pallas_call(
            functools.partial(layer, n),
            out_shape=jax.ShapeDtypeStruct((rows * d // 128, 128), BF16),
            in_specs=[any_, any_, any_, vmem, any_, any_, vmem, any_, any_, any_, vmem, vmem],
            out_specs=vmem,
            scratch_shapes=[
                pltpu.VMEM((SLOTS, DEEP, WIDE), BF16),
                pltpu.VMEM((rows, d), BF16),
                pltpu.VMEM((rows, d), BF16),
                pltpu.VMEM((rows * d // 128, 128), BF16),
                pltpu.VMEM((rows * d // 128, 128), F32),
                pltpu.VMEM((rows, ff), BF16),
                pltpu.VMEM((rows * 8, head), F32),
                pltpu.VMEM((rows * 8, head), F32),
                pltpu.VMEM((chunks, far, 128, 128), BF16),
                pltpu.VMEM((chunks, near, 128, 128), BF16),
                pltpu.VMEM((groups, far, rows, 128), BF16),
                pltpu.VMEM((groups, near, rows, 128), BF16),
                pltpu.VMEM((far, 128, 128), BF16),
                pltpu.VMEM((near, 128, 128), BF16),
                pltpu.VMEM((far, rows, 128), BF16),
                pltpu.VMEM((near, rows, 128), BF16),
                dma((SLOTS,)),
                dma(()),
                dma((2 * (far + near),)),
                dma((2 * (far + near),)),
                dma((chunks, far)), dma((chunks, near)),
                dma((groups, far)), dma((groups, near)),
                dma((chunks, far)), dma((chunks, near)),
                dma((groups, far)), dma((groups, near)),
            ],
            compiler_params=pltpu.CompilerParams(collective_id=0, has_side_effects=True, vmem_limit_bytes=67043328),
            name="decoder_layer",
        )(x, k_cache.reshape(batch, keys, head), v_cache.reshape(batch, keys, head), gain_a.astype(F32)[None], wq, wo,
          gain_m.astype(F32)[None], w_gate, w_up, w_down, cos, sin)
        return out.reshape(d // 128, rows, 128).transpose(1, 0, 2).reshape(rows, d)

    states, cache, columns, rows_of = P("dp", None), P("dp", None, "tp", None), P(None, "tp"), P("tp", None)
    return jax.shard_map(
        step,
        mesh=mesh,
        in_specs=(states, cache, cache, P(None), columns, rows_of, P(None), columns, columns, rows_of),
        out_specs=states,
        check_vma=False,
    )
```

```python
import functools

import jax
import jax.numpy as jnp
import numpy as np
from jax import lax
from jax.experimental import pallas as pl
from jax.experimental.pallas import tpu as pltpu
from jax.sharding import PartitionSpec as P

HEAD = 128
THETA = 10000
F32, BF16 = jnp.float32, jnp.bfloat16

DEEP, WIDE = 4096, 256
SLOTS = 24
HELD = 8


def mult(v, k):
    return pl.multiple_of(v, k)


def layer(n, x_hbm, kc, vc, gain_a_hbm, wq, wo, gain_m_hbm, wg, wu, wd, trig_hbm, out,
          ring, x, ab, states, y, part, hidden, q3, seen3, gain_a, gain_m, trig, box1, box2, stage1, stage2,
          slot_sem, x_sem, out_sem, send1, send2, recv1, recv2):
    me = lax.axis_index("tp")
    rows, d = x_hbm.shape
    head = kc.shape[2]
    keys = kc.shape[1]
    up_blocks = wg.shape[1] // WIDE
    down_rows = wd.shape[0]
    down_blocks = d // WIDE
    mlp = 4 * up_blocks + down_blocks
    chunk_rows = 16
    chunks = rows // chunk_rows

    def put(src, dst, slot):
        pltpu.make_async_copy(src, dst, slot_sem.at[slot]).start()

    def ready(slot, deep=DEEP):
        pltpu.make_async_copy(wg.at[pl.ds(0, deep), pl.ds(0, WIDE)], ring.at[slot, pl.ds(0, deep)], slot_sem.at[slot]).wait()

    def start_wq(cb, part_):
        slot = 2 * cb + part_
        put(wq.at[pl.ds(part_ * DEEP, DEEP), pl.ds(mult(cb * WIDE, WIDE), WIDE)], ring.at[slot], slot)

    def start_wo(cb):
        slot = HELD + cb
        for j in range(4):
            put(wo.at[:, pl.ds(mult(cb * 4 * WIDE + j * WIDE, WIDE), WIDE)], ring.at[slot, pl.ds(j * 1024, 1024)], slot)

    def kv_slot(j):
        return lax.rem(2 * HELD + lax.rem(j, SLOTS - HELD), SLOTS)

    def start_kv(it):
        for which, src in enumerate((kc, vc)):
            slot = kv_slot(2 * it + which)
            for p in range(2):
                for side in range(2):
                    put(src.at[it * 4 + 2 * p + side], ring.at[slot, pl.ds(p * keys, keys), pl.ds(side * head, head)], slot)

    def mlp_slot(m):
        return lax.rem(2 * HELD + m, SLOTS)

    def start_mlp4(m):
        @pl.when(m < 4 * up_blocks)
        def _():
            col = pl.ds(mult(m // 4 * WIDE, WIDE), WIDE)
            for r in range(4):
                slot = mlp_slot(m + r)
                put((wg, wu)[r // 2].at[pl.ds(r % 2 * DEEP, DEEP), col], ring.at[slot], slot)

        @pl.when((m >= 4 * up_blocks) & (m < mlp))
        def _():
            for r in range(4):
                slot = mlp_slot(m + r)
                nb = m + r - 4 * up_blocks
                put(wd.at[:, pl.ds(mult(nb * WIDE, WIDE), WIDE)], ring.at[slot, pl.ds(0, down_rows)], slot)

    small = [pltpu.make_async_copy(a, b, x_sem.at[i]) for i, (a, b) in enumerate(
        ((x_hbm, x), (gain_a_hbm, gain_a), (gain_m_hbm, gain_m), (trig_hbm, trig)))]
    for copy in small:
        copy.start()
    for cb in range(2):
        for part_ in range(2):
            start_wq(cb, part_)
    barrier = pltpu.get_barrier_semaphore()
    for step in (1, 2, n - 2, n - 1):
        pl.semaphore_signal(barrier, inc=1, device_id={"tp": lax.rem(me + step, n)}, device_id_type=pl.DeviceIdType.MESH)

    def steps(s, g, piece_rows, box, stage, send, recv, whole, residual, done):
        sign = 1 - 2 * lax.rem(g + lax.axis_index("dp"), 2)

        def dev(k):
            return lax.rem(me + k * sign + 2 * n, n)

        def at(o):
            return pl.ds(mult((g * n + o) * piece_rows, piece_rows), piece_rows)

        def remote(i, src, dst, to):
            return pltpu.make_async_remote_copy(src_ref=src, dst_ref=dst, send_sem=send.at[i], recv_sem=recv.at[g, i],
                                                device_id={"tp": dev(to)}, device_id_type=pl.DeviceIdType.MESH)

        def term(i, to):
            return remote(i, stage.at[i], box.at[g, i], to)

        def piece(i, owner, to):
            ref = whole.at[at(dev(owner))]
            return remote(7 + i, ref, ref, to)

        def go(copy):
            @pl.when(g > 0)
            def _():
                copy.wait_send()

            copy.start()

        def send_term(i, owner, to, *terms):
            value = part[at(dev(owner)), :]
            for k in terms:
                term(k, 0).wait_recv()
                value = value + box[g, k].astype(F32)
            copy = term(i, to)

            @pl.when(g > 0)
            def _():
                copy.wait_send()

            stage[i] = value.astype(BF16)
            copy.start()

        def forward(k, i, owner, to):
            piece(k, owner, 0).wait_recv()
            go(piece(i, owner, to))

        if s == 0:
            send_term(0, 4, 1)
            send_term(2, -3, -1)
            send_term(1, 1, 1)
        if s == 1:
            send_term(3, 3, 1, 0)
            send_term(4, -2, -1, 2)
        if s == 2:
            send_term(5, 2, 2, 3)
            send_term(6, -1, -1, 4)
        if s == 3:
            value = part[at(me), :]
            for k in (1, 5, 6):
                term(k, 0).wait_recv()
                value = value + box[g, k].astype(F32)
            whole[at(me), :] = (residual(g) + value).astype(BF16)
            for i, to in ((1, 2), (2, -1), (0, 1)):
                go(piece(i, 0, to))
        if s == 4:
            forward(1, 3, -2, 1)
            forward(2, 4, 1, -1)
        if s == 5:
            forward(3, 5, -3, 1)
            forward(4, 6, 2, -1)
        if s == 6:
            for i, owner in ((0, -1), (5, -4), (6, 3)):
                piece(i, owner, 0).wait_recv()
            done(g)
        if s == 7:
            for i in range(7):
                term(i, 1).wait_send()
                piece(i, 0, 1).wait_send()

    LAST = 6

    blocks = d // 128

    def norm_x(i, _):
        r = pl.ds(mult(i * 16, 16), 16)
        total = jnp.zeros((16, 128), F32)
        for k in range(blocks):
            wide = x[r, pl.ds(k * 128, 128)].astype(F32)
            total = total + wide * wide
        scale = lax.rsqrt(jnp.sum(total, -1, keepdims=True) * (1.0 / d) + 1e-6)
        for k in range(blocks):
            c = pl.ds(k * 128, 128)
            ab[r, c] = (x[r, c].astype(F32) * scale * gain_a[k:k + 1, :].astype(F32)).astype(BF16)
        return 0

    for copy in small:
        copy.wait()
    for cb in (2, 3):
        for part_ in range(2):
            start_wq(cb, part_)
    start_kv(0)
    with jax.named_scope("norm"):
        lax.fori_loop(0, rows // 16, norm_x, 0)
    for it in range(1, 4):
        start_kv(it)

    def project(cb, _):
        ready(2 * cb)
        ready(2 * cb + 1)
        acc = jnp.dot(ab[:, pl.ds(0, DEEP)], ring[2 * cb], preferred_element_type=F32)
        acc = acc + jnp.dot(ab[:, pl.ds(DEEP, DEEP)], ring[2 * cb + 1], preferred_element_type=F32)
        for j in range(2):
            t = acc[:, j * head:(j + 1) * head].astype(BF16).astype(F32)
            t = t * trig[0:1, :] + pltpu.roll(t, head // 2, 1) * trig[1:2, :]
            q3[pl.ds(2 * cb + j, rows, stride=8), :] = t.astype(BF16).astype(F32)
        start_kv(4 + cb)
        start_wo(2 * cb)
        start_wo(2 * cb + 1)
        return 0

    with jax.named_scope("project"):
        lax.fori_loop(0, 4, project, 0)
    pl.semaphore_wait(barrier, 4)

    def residual1(g):
        r = pl.ds(mult(g * chunk_rows, chunk_rows), chunk_rows)
        cols = [x[r, pl.ds(mult(me * 1024 + k * 128, 128), 128)].astype(F32) for k in range(8)]
        return jnp.concatenate(cols, 0)

    def done1(g):
        total = jnp.zeros((chunk_rows, 128), F32)
        for k in range(blocks):
            wide = states[pl.ds(mult(g * 1024 + k * 16, 16), 16), :].astype(F32)
            total = total + wide * wide
        scale = lax.rsqrt(jnp.sum(total, -1, keepdims=True) * (1.0 / d) + 1e-6)
        r = pl.ds(mult(g * chunk_rows, chunk_rows), chunk_rows)
        for k in range(blocks):
            c = pl.ds(k * 128, 128)
            wide = states[pl.ds(mult(g * 1024 + k * 16, 16), 16), :].astype(F32)
            ab[r, c] = (wide * scale * gain_m[k:k + 1, :].astype(F32)).astype(BF16)

    first = functools.partial(steps, piece_rows=chunk_rows * 8, box=box1, stage=stage1, send=send1, recv=recv1,
                              whole=states, residual=residual1, done=done1)

    def tick1(t):
        for s in [0] + list(range(1, LAST + 1)):
            since = t - s

            @pl.when((since == 0) | (since == 2) | (since == 4))
            def _():
                with jax.named_scope(f"a{s}"):
                    begin = jnp.where(since == 0, 0, 1 + since // 2)
                    lax.fori_loop(begin, 2 + since // 2, lambda g, _: (first(s, g), 0)[1], 0)

    def attend(it):
        ks, vs = kv_slot(2 * it), kv_slot(2 * it + 1)
        ready(ks)
        ready(vs)
        zero = jnp.zeros((8, head), F32)
        weights = []
        for p in range(2):
            s0 = (it * 4 + 2 * p) * 8
            q = jnp.concatenate([jnp.concatenate([q3[pl.ds(mult(s0, 8), 8), :], zero], 1),
                                 jnp.concatenate([zero, q3[pl.ds(mult(s0 + 8, 8), 8), :]], 1)], 0).astype(BF16)
            scores = lax.dot_general(q, ring[ks, pl.ds(p * keys, keys)], (((1,), (1,)), ((), ())),
                                     preferred_element_type=F32) * head**-0.5
            e = jnp.exp(scores - jnp.max(scores, -1, keepdims=True))
            weights.append((e * (1.0 / jnp.sum(e, -1, keepdims=True))).astype(BF16))
        for p in range(2):
            s0 = (it * 4 + 2 * p) * 8
            o = jnp.dot(weights[p], ring[vs, pl.ds(p * keys, keys)], preferred_element_type=F32)
            o = o.astype(BF16).astype(F32)
            seen3[pl.ds(mult(s0, 8), 8), :] = o[:8, :head]
            seen3[pl.ds(mult(s0 + 8, 8), 8), :] = o[8:, head:]

        @pl.when(it < 8)
        def _():
            start_kv(it + 8)

    def wo_pass(row0, count):
        seen = jnp.concatenate([seen3[pl.ds(row0 * 8 + h, count, stride=8), :] for h in range(8)], 1).astype(BF16)

        def columns(cb2, _):
            for k in range(2):
                @pl.when(row0 == 0)
                def _():
                    ready(HELD + 2 * cb2 + k)

            for k in range(2):
                cb = 2 * cb2 + k
                for j in range(4):
                    acc = jnp.dot(seen, ring[HELD + cb, pl.ds(j * 1024, 1024)], preferred_element_type=F32)
                    for r in range(count // 16):
                        base = ((row0 // 16 + r) * 8 + cb) * 128 + j * 32
                        part[pl.ds(mult(base, 16), 16), :] = acc[r * 16:(r + 1) * 16, :128]
                        part[pl.ds(mult(base + 16, 16), 16), :] = acc[r * 16:(r + 1) * 16, 128:]
            return 0

        with jax.named_scope("wo"):
            lax.fori_loop(0, 4, columns, 0)

    def sequences(it, _):
        with jax.named_scope("attend"):
            attend(it)

        @pl.when((lax.rem(it, 2) == 1) & (it >= 8))
        def _():
            start_mlp4(2 * (it - 1 - 8))

        @pl.when(it == 7)
        def _():
            wo_pass(0, 32)

        @pl.when((it == 11) | (it == 15))
        def _():
            wo_pass((it - 3) * 4, 16)

        @pl.when((lax.rem(it, 2) == 1) & (it >= 7))
        def _():
            tick1((it - 7) // 2)
        return 0

    lax.fori_loop(0, 16, sequences, 0)
    start_mlp4(16)
    start_mlp4(20)

    def rest1(t, _):
        tick1(t)
        return 0

    lax.fori_loop(5, 5 + LAST, rest1, 0)

    def gate_up(cb, _):
        m = 4 * cb
        outs = []
        for r in range(4):
            ready(mlp_slot(m + r))
        for r in range(2):
            s0, s1 = mlp_slot(m + 2 * r), mlp_slot(m + 2 * r + 1)
            acc = jnp.dot(ab[:, pl.ds(0, DEEP)], ring[s0], preferred_element_type=F32)
            outs.append(acc + jnp.dot(ab[:, pl.ds(DEEP, DEEP)], ring[s1], preferred_element_type=F32))
        hidden[:, pl.ds(mult(cb * WIDE, WIDE), WIDE)] = (jax.nn.silu(outs[0]) * outs[1]).astype(BF16)
        start_mlp4(m + SLOTS)
        return 0

    with jax.named_scope("gate_up"):
        lax.fori_loop(0, up_blocks, gate_up, 0)

    def residual2(g):
        pieces = [states[pl.ds(mult(c * 1024 + g * 128 + me * 16, 16), 16), :] for c in range(chunks)]
        return jnp.concatenate(pieces, 0).astype(F32)

    groups = d // 1024

    def done2(g):
        for o in range(n):
            p = g * n + o
            pltpu.make_async_copy(y.at[pl.ds(mult(p * rows, rows), rows)], out.at[:, pl.ds(mult(p * 128, 128), 128)], out_sem.at[g]).start()

    second = functools.partial(steps, piece_rows=rows, box=box2, stage=stage2, send=send2, recv=recv2,
                               whole=y, residual=residual2, done=done2)

    def down(t, _):
        @pl.when(t < groups)
        def _():
            with jax.named_scope("down"):
                for i in range(4):
                    ready(mlp_slot(4 * up_blocks + 4 * t + i), down_rows)
                for i in range(4):
                    nb = 4 * t + i
                    slot = mlp_slot(4 * up_blocks + nb)
                    acc = jnp.dot(hidden[...], ring[slot, pl.ds(0, down_rows)], preferred_element_type=F32)
                    part[pl.ds(mult(nb * 2 * rows, rows), rows), :] = acc[:, :128]
                    part[pl.ds(mult(nb * 2 * rows + rows, rows), rows), :] = acc[:, 128:]
            start_mlp4(4 * up_blocks + 4 * t + SLOTS)

        for s in [0] + list(range(LAST, 0, -1)):
            @pl.when((t >= 2 * s) & (t - 2 * s < groups))
            def _():
                with jax.named_scope(f"b{s}"):
                    second(s, t - 2 * s)
        return 0

    lax.fori_loop(0, groups + 2 * LAST, down, 0)
    first(LAST + 1, chunks - 1)
    second(LAST + 1, groups - 1)
    for g in range(groups):
        piece = y.at[pl.ds(0, n * rows)]
        pltpu.make_async_copy(piece, piece, out_sem.at[g]).wait()


def solution(mesh):
    n = mesh.shape["tp"]

    def step(x, k_cache, v_cache, gain_a, wq, wo, gain_m, w_gate, w_up, w_down):
        rows, d = x.shape
        batch, keys, _, head = k_cache.shape
        ff = w_gate.shape[1]
        half = head // 2
        angle = np.float32(keys - 1) * THETA ** (-np.arange(half) / half)
        cos, sin = np.cos(angle), np.sin(angle)
        trig = jnp.asarray(np.stack([np.concatenate([cos, cos]), np.concatenate([-sin, sin])]), F32)
        any_ = pl.BlockSpec(memory_space=pl.ANY)
        chunks, groups = rows // 16, d // 1024
        dma = pltpu.SemaphoreType.DMA
        out = pl.pallas_call(
            functools.partial(layer, n),
            out_shape=jax.ShapeDtypeStruct((rows, d), BF16),
            in_specs=[any_] * 11,
            out_specs=any_,
            scratch_shapes=[
                pltpu.VMEM((SLOTS, DEEP, WIDE), BF16),
                pltpu.VMEM((rows, d), BF16),
                pltpu.VMEM((rows, d), BF16),
                pltpu.VMEM((rows * d // 128, 128), BF16),
                pltpu.VMEM((rows * d // 128, 128), BF16),
                pltpu.VMEM((rows * d // 128, 128), F32),
                pltpu.VMEM((rows, ff), BF16),
                pltpu.VMEM((rows * 8, head), F32),
                pltpu.VMEM((rows * 8, head), F32),
                pltpu.VMEM((d // 128, 128), BF16),
                pltpu.VMEM((d // 128, 128), BF16),
                pltpu.VMEM((2, 128), F32),
                pltpu.VMEM((chunks, 7, 128, 128), BF16),
                pltpu.VMEM((groups, 7, rows, 128), BF16),
                pltpu.VMEM((7, 128, 128), BF16),
                pltpu.VMEM((7, rows, 128), BF16),
                dma((SLOTS,)),
                dma((4,)),
                dma((groups,)),
                dma((14,)),
                dma((14,)),
                dma((chunks, 14)),
                dma((groups, 14)),
            ],
            compiler_params=pltpu.CompilerParams(collective_id=0, has_side_effects=True, vmem_limit_bytes=67043328),
            name="decoder_layer",
        )(x, k_cache.reshape(batch, keys, head), v_cache.reshape(batch, keys, head), gain_a.reshape(d // 128, 128), wq, wo,
          gain_m.reshape(d // 128, 128), w_gate, w_up, w_down, trig)
        return out

    states, cache, columns, rows_of = P("dp", None), P("dp", None, "tp", None), P(None, "tp"), P("tp", None)
    return jax.shard_map(
        step,
        mesh=mesh,
        in_specs=(states, cache, cache, P(None), columns, rows_of, P(None), columns, columns, rows_of),
        out_specs=states,
        check_vma=False,
    )
```

```python
import functools

import jax
import jax.numpy as jnp
import numpy as np
from jax import lax
from jax.experimental import pallas as pl
from jax.experimental.pallas import tpu as pltpu
from jax.sharding import PartitionSpec as P

HEAD = 128
THETA = 10000
F32, BF16 = jnp.float32, jnp.bfloat16

DEEP, WIDE = 4096, 256
SLOTS = 24
LIMIT = 62 * 2**20
HELD = 8


def mult(v, k):
    return pl.multiple_of(v, k)


def layer(n, x_hbm, kc, vc, gain_a_hbm, wq, wo, gain_m_hbm, wg, wu, wd, trig_hbm, y,
          ring, x, ab, states, part, hidden, q3, seen3, gain_a, gain_m, trig, box1, box2, stage1, stage2,
          slot_sem, x_sem, send1, send2, recv1, recv2):
    me = lax.axis_index("tp")
    rows, d = x_hbm.shape
    head = kc.shape[2]
    keys = kc.shape[1]
    up_blocks = wg.shape[1] // WIDE
    down_rows = wd.shape[0]
    down_blocks = d // WIDE
    mlp = 4 * up_blocks + down_blocks
    chunk_rows = 16
    chunks = rows // chunk_rows

    def put(src, dst, slot):
        pltpu.make_async_copy(src, dst, slot_sem.at[slot]).start()

    def ready(slot, deep=DEEP):
        pltpu.make_async_copy(wg.at[pl.ds(0, deep), pl.ds(0, WIDE)], ring.at[slot, pl.ds(0, deep)], slot_sem.at[slot]).wait()

    def start_wq(cb, part_):
        slot = 2 * cb + part_
        put(wq.at[pl.ds(part_ * DEEP, DEEP), pl.ds(mult(cb * WIDE, WIDE), WIDE)], ring.at[slot], slot)

    def start_wo(cb):
        slot = HELD + cb
        for j in range(4):
            put(wo.at[:, pl.ds(mult(cb * 4 * WIDE + j * WIDE, WIDE), WIDE)], ring.at[slot, pl.ds(j * 1024, 1024)], slot)

    def kv_slot(j):
        return lax.rem(2 * HELD + lax.rem(j, SLOTS - HELD), SLOTS)

    def start_kv(it):
        for which, src in enumerate((kc, vc)):
            slot = kv_slot(2 * it + which)
            for p in range(2):
                for side in range(2):
                    put(src.at[it * 4 + 2 * p + side], ring.at[slot, pl.ds(p * keys, keys), pl.ds(side * head, head)], slot)

    def mlp_slot(m):
        return lax.rem(2 * HELD + m, SLOTS)

    def start_mlp4(m):
        @pl.when(m < 4 * up_blocks)
        def _():
            col = pl.ds(mult(m // 4 * WIDE, WIDE), WIDE)
            for r in range(4):
                slot = mlp_slot(m + r)
                put((wg, wu)[r // 2].at[pl.ds(r % 2 * DEEP, DEEP), col], ring.at[slot], slot)

        @pl.when((m >= 4 * up_blocks) & (m < mlp))
        def _():
            for r in range(4):
                slot = mlp_slot(m + r)
                nb = m + r - 4 * up_blocks
                put(wd.at[:, pl.ds(mult(nb * WIDE, WIDE), WIDE)], ring.at[slot, pl.ds(0, down_rows)], slot)

    small = [pltpu.make_async_copy(a, b, x_sem.at[i]) for i, (a, b) in enumerate(
        ((x_hbm, x), (gain_a_hbm, gain_a), (gain_m_hbm, gain_m), (trig_hbm, trig)))]
    for copy in small:
        copy.start()
    for cb in range(2):
        for part_ in range(2):
            start_wq(cb, part_)
    barrier = pltpu.get_barrier_semaphore()
    for step in (1, 2, n - 2, n - 1):
        pl.semaphore_signal(barrier, inc=1, device_id={"tp": lax.rem(me + step, n)}, device_id_type=pl.DeviceIdType.MESH)

    def steps(s, g, piece_rows, box, stage, send, recv, whole, residual, done):
        sign = 1 - 2 * lax.rem(g + lax.axis_index("dp"), 2)

        def dev(k):
            return lax.rem(me + k * sign + 2 * n, n)

        def at(o):
            return pl.ds(mult((g * n + o) * piece_rows, piece_rows), piece_rows)

        def remote(i, src, dst, to):
            return pltpu.make_async_remote_copy(src_ref=src, dst_ref=dst, send_sem=send.at[g, i], recv_sem=recv.at[g, i],
                                                device_id={"tp": dev(to)}, device_id_type=pl.DeviceIdType.MESH)

        def term(i, to):
            return remote(i, stage.at[g, i], box.at[g, i], to)

        def piece(i, owner, to):
            ref = whole.at[at(dev(owner))]
            return remote(7 + i, ref, ref, to)

        def send_term(i, owner, to, *terms):
            value = part[at(dev(owner)), :]
            for k in terms:
                term(k, 0).wait_recv()
                value = value + box[g, k].astype(F32)
            stage[g, i] = value.astype(BF16)
            term(i, to).start()

        if s == 0:
            send_term(0, 4, 2)
            send_term(1, 3, 1)
            send_term(3, -3, -1)
            send_term(2, 1, 1)
            send_term(4, -1, -1)
        if s == 1:
            send_term(6, -2, -2, 3)
            send_term(5, 2, 2, 1, 0)
        if s == 2:
            value = part[at(me), :]
            for k in (2, 4, 6, 5):
                term(k, 0).wait_recv()
                value = value + box[g, k].astype(F32)
            whole[at(me), :] = (residual(g) + value).astype(BF16)
            for i, to in ((0, 2), (2, -2), (1, 1), (3, -1)):
                piece(i, 0, to).start()
        if s == 3:
            piece(2, 2, 0).wait_recv()
            piece(6, 2, -1).start()
            piece(0, -2, 0).wait_recv()
            piece(4, -2, 2).start()
            piece(5, -2, 1).start()
        if s == 4:
            for i, owner in ((1, -1), (3, 1), (4, -4), (5, -3), (6, 3)):
                piece(i, owner, 0).wait_recv()
            done(g)
        if s == 5:
            for i in range(7):
                term(i, 1).wait_send()
                piece(i, 0, 1).wait_send()

    LAST = 4

    blocks = d // 128

    def norm_x(i, _):
        r = pl.ds(mult(i * 16, 16), 16)
        total = jnp.zeros((16, 128), F32)
        for k in range(blocks):
            wide = x[r, pl.ds(k * 128, 128)].astype(F32)
            total = total + wide * wide
        scale = lax.rsqrt(jnp.sum(total, -1, keepdims=True) * (1.0 / d) + 1e-6)
        for k in range(blocks):
            c = pl.ds(k * 128, 128)
            ab[r, c] = (x[r, c].astype(F32) * scale * gain_a[k:k + 1, :].astype(F32)).astype(BF16)
        return 0

    for copy in small:
        copy.wait()
    for cb in (2, 3):
        for part_ in range(2):
            start_wq(cb, part_)
    start_kv(0)
    with jax.named_scope("norm"):
        lax.fori_loop(0, rows // 16, norm_x, 0)
    for it in range(1, 4):
        start_kv(it)

    def project(cb, _):
        ready(2 * cb)
        ready(2 * cb + 1)
        acc = jnp.dot(ab[:, pl.ds(0, DEEP)], ring[2 * cb], preferred_element_type=F32)
        acc = acc + jnp.dot(ab[:, pl.ds(DEEP, DEEP)], ring[2 * cb + 1], preferred_element_type=F32)
        for j in range(2):
            t = acc[:, j * head:(j + 1) * head].astype(BF16).astype(F32)
            t = t * trig[0:1, :] + pltpu.roll(t, head // 2, 1) * trig[1:2, :]
            q3[pl.ds(2 * cb + j, rows, stride=8), :] = t.astype(BF16).astype(F32)
        start_kv(4 + cb)
        start_wo(2 * cb)
        start_wo(2 * cb + 1)
        return 0

    with jax.named_scope("project"):
        lax.fori_loop(0, 4, project, 0)
    pl.semaphore_wait(barrier, 4)

    def residual1(g):
        r = pl.ds(mult(g * chunk_rows, chunk_rows), chunk_rows)
        cols = [x[r, pl.ds(mult(me * 1024 + k * 128, 128), 128)].astype(F32) for k in range(8)]
        return jnp.concatenate(cols, 0)

    def done1(g):
        total = jnp.zeros((chunk_rows, 128), F32)
        for k in range(blocks):
            wide = states[pl.ds(mult(g * 1024 + k * 16, 16), 16), :].astype(F32)
            total = total + wide * wide
        scale = lax.rsqrt(jnp.sum(total, -1, keepdims=True) * (1.0 / d) + 1e-6)
        r = pl.ds(mult(g * chunk_rows, chunk_rows), chunk_rows)
        for k in range(blocks):
            c = pl.ds(k * 128, 128)
            wide = states[pl.ds(mult(g * 1024 + k * 16, 16), 16), :].astype(F32)
            ab[r, c] = (wide * scale * gain_m[k:k + 1, :].astype(F32)).astype(BF16)

    first = functools.partial(steps, piece_rows=chunk_rows * 8, box=box1, stage=stage1, send=send1, recv=recv1,
                              whole=states, residual=residual1, done=done1)

    def attend(it):
        ks, vs = kv_slot(2 * it), kv_slot(2 * it + 1)
        ready(ks)
        ready(vs)
        zero = jnp.zeros((8, head), F32)
        weights = []
        for p in range(2):
            s0 = (it * 4 + 2 * p) * 8
            q = jnp.concatenate([jnp.concatenate([q3[pl.ds(mult(s0, 8), 8), :], zero], 1),
                                 jnp.concatenate([zero, q3[pl.ds(mult(s0 + 8, 8), 8), :]], 1)], 0).astype(BF16)
            scores = lax.dot_general(q, ring[ks, pl.ds(p * keys, keys)], (((1,), (1,)), ((), ())),
                                     preferred_element_type=F32) * head**-0.5
            e = jnp.exp(scores - jnp.max(scores, -1, keepdims=True))
            weights.append((e * (1.0 / jnp.sum(e, -1, keepdims=True))).astype(BF16))
        for p in range(2):
            s0 = (it * 4 + 2 * p) * 8
            o = jnp.dot(weights[p], ring[vs, pl.ds(p * keys, keys)], preferred_element_type=F32)
            o = o.astype(BF16).astype(F32)
            seen3[pl.ds(mult(s0, 8), 8), :] = o[:8, :head]
            seen3[pl.ds(mult(s0 + 8, 8), 8), :] = o[8:, head:]

        @pl.when(it < 8)
        def _():
            start_kv(it + 8)

    def wo_pass(row0, count):
        seen = jnp.concatenate([seen3[pl.ds(row0 * 8 + h, count, stride=8), :] for h in range(8)], 1).astype(BF16)

        def columns(cb2, _):
            for k in range(2):
                @pl.when(row0 == 0)
                def _():
                    ready(HELD + 2 * cb2 + k)

            for k in range(2):
                cb = 2 * cb2 + k
                for j in range(4):
                    acc = jnp.dot(seen, ring[HELD + cb, pl.ds(j * 1024, 1024)], preferred_element_type=F32)
                    for r in range(count // 16):
                        base = ((row0 // 16 + r) * 8 + cb) * 128 + j * 32
                        part[pl.ds(mult(base, 16), 16), :] = acc[r * 16:(r + 1) * 16, :128]
                        part[pl.ds(mult(base + 16, 16), 16), :] = acc[r * 16:(r + 1) * 16, 128:]
            return 0

        with jax.named_scope("wo"):
            lax.fori_loop(0, 4, columns, 0)

    def sequences(it, _):
        with jax.named_scope("attend"):
            attend(it)

        @pl.when((lax.rem(it, 2) == 1) & (it >= 8))
        def _():
            start_mlp4(2 * (it - 1 - 8))

        @pl.when(it == 9)
        def _():
            wo_pass(0, 32)
            lax.fori_loop(0, 2, run1(0), 0)

        @pl.when(it == 13)
        def _():
            lax.fori_loop(0, 2, run1(1), 0)

        @pl.when((it == 12) | (it == 15))
        def _():
            c = (it - 6) // 3
            wo_pass(c * 16, 16)
            run1(0)(c, 0)
        return 0

    def run1(s):
        def body(g, _):
            with jax.named_scope(f"a{s}"):
                first(s, g)
            return 0
        return body

    lax.fori_loop(0, 16, sequences, 0)
    start_mlp4(16)
    start_mlp4(20)

    for s, lo, hi in ((1, 2, 3), (2, 0, 2), (1, 3, 4), (2, 2, 3), (3, 0, 2), (2, 3, 4), (3, 2, 3), (4, 0, 2), (3, 3, 4), (4, 2, 4)):
        lax.fori_loop(lo, hi, run1(s), 0)

    def gate_up(cb, _):
        m = 4 * cb
        outs = []
        for r in range(4):
            ready(mlp_slot(m + r))
        for r in range(2):
            s0, s1 = mlp_slot(m + 2 * r), mlp_slot(m + 2 * r + 1)
            acc = jnp.dot(ab[:, pl.ds(0, DEEP)], ring[s0], preferred_element_type=F32)
            outs.append(acc + jnp.dot(ab[:, pl.ds(DEEP, DEEP)], ring[s1], preferred_element_type=F32))
        hidden[:, pl.ds(mult(cb * WIDE, WIDE), WIDE)] = (jax.nn.silu(outs[0]) * outs[1]).astype(BF16)
        start_mlp4(m + SLOTS)
        return 0

    with jax.named_scope("gate_up"):
        lax.fori_loop(0, up_blocks, gate_up, 0)

    def residual2(g):
        pieces = [states[pl.ds(mult(c * 1024 + g * 128 + me * 16, 16), 16), :] for c in range(chunks)]
        return jnp.concatenate(pieces, 0).astype(F32)

    groups = d // 1024

    second = functools.partial(steps, piece_rows=rows, box=box2, stage=stage2, send=send2, recv=recv2,
                               whole=y, residual=residual2, done=lambda g: None)

    def run2(s):
        def body(g, _):
            with jax.named_scope(f"b{s}"):
                second(s, g)
            return 0
        return body

    def down(t, _):
        with jax.named_scope("down"):
            for i in range(4):
                ready(mlp_slot(4 * up_blocks + 4 * t + i), down_rows)
            for i in range(4):
                nb = 4 * t + i
                slot = mlp_slot(4 * up_blocks + nb)
                acc = jnp.dot(hidden[...], ring[slot, pl.ds(0, down_rows)], preferred_element_type=F32)
                part[pl.ds(mult(nb * 2 * rows, rows), rows), :] = acc[:, :128]
                part[pl.ds(mult(nb * 2 * rows + rows, rows), rows), :] = acc[:, 128:]
        start_mlp4(4 * up_blocks + 4 * t + SLOTS)
        for s, lag in enumerate(LAGS):
            @pl.when(t >= lag)
            def _():
                run2(s)(t - lag, 0)
        return 0

    LAGS = (0, 2, 5, 7)
    lax.fori_loop(0, groups, down, 0)
    for s, g in ((2, 3), (3, 1), (2, 4), (1, 6), (3, 2), (1, 7), (2, 5), (3, 3), (2, 6), (3, 4), (2, 7), (3, 5), (3, 6), (3, 7)):
        run2(s)(jnp.int32(g), 0)
    lax.fori_loop(0, groups, run2(LAST), 0)
    lax.fori_loop(0, chunks, lambda g, _: (first(LAST + 1, g), 0)[1], 0)
    lax.fori_loop(0, groups, lambda g, _: (second(LAST + 1, g), 0)[1], 0)


def place(y, out, sem):
    rows, d = out.shape

    def copy(p):
        return pltpu.make_async_copy(y.at[pl.ds(mult(p * rows, rows), rows)], out.at[:, pl.ds(mult(p * 128, 128), 128)], sem)

    lax.fori_loop(0, d // 128, lambda p, _: (copy(p).start(), 0)[1], 0)
    pltpu.make_async_copy(y, y, sem).wait()


def solution(mesh):
    n = mesh.shape["tp"]

    def step(x, k_cache, v_cache, gain_a, wq, wo, gain_m, w_gate, w_up, w_down):
        rows, d = x.shape
        batch, keys, _, head = k_cache.shape
        ff = w_gate.shape[1]
        half = head // 2
        angle = np.float32(keys - 1) * THETA ** (-np.arange(half) / half)
        cos, sin = np.cos(angle), np.sin(angle)
        trig = jnp.asarray(np.stack([np.concatenate([cos, cos]), np.concatenate([-sin, sin])]), F32)
        any_ = pl.BlockSpec(memory_space=pl.ANY)
        chunks, groups = rows // 16, d // 1024
        dma = pltpu.SemaphoreType.DMA
        pieces = pl.pallas_call(
            functools.partial(layer, n),
            out_shape=pltpu.VMEM((rows * d // 128, 128), BF16),
            in_specs=[any_] * 11,
            out_specs=pl.BlockSpec(memory_space=pltpu.VMEM),
            scratch_shapes=[
                pltpu.VMEM((SLOTS, DEEP, WIDE), BF16),
                pltpu.VMEM((rows, d), BF16),
                pltpu.VMEM((rows, d), BF16),
                pltpu.VMEM((rows * d // 128, 128), BF16),
                pltpu.VMEM((rows * d // 128, 128), F32),
                pltpu.VMEM((rows, ff), BF16),
                pltpu.VMEM((rows * 8, head), F32),
                pltpu.VMEM((rows * 8, head), F32),
                pltpu.VMEM((d // 128, 128), BF16),
                pltpu.VMEM((d // 128, 128), BF16),
                pltpu.VMEM((2, 128), F32),
                pltpu.VMEM((chunks, 7, 128, 128), BF16),
                pltpu.VMEM((groups, 7, rows, 128), BF16),
                pltpu.VMEM((chunks, 7, 128, 128), BF16),
                pltpu.VMEM((groups, 7, rows, 128), BF16),
                dma((SLOTS,)),
                dma((4,)),
                dma((chunks, 14)),
                dma((groups, 14)),
                dma((chunks, 14)),
                dma((groups, 14)),
            ],
            compiler_params=pltpu.CompilerParams(collective_id=0, has_side_effects=True, vmem_limit_bytes=LIMIT),
            name="decoder_layer",
        )(x, k_cache.reshape(batch, keys, head), v_cache.reshape(batch, keys, head), gain_a.reshape(d // 128, 128), wq, wo,
          gain_m.reshape(d // 128, 128), w_gate, w_up, w_down, trig)
        return pl.pallas_call(
            place,
            out_shape=jax.ShapeDtypeStruct((rows, d), BF16),
            in_specs=[pl.BlockSpec(memory_space=pltpu.VMEM)],
            out_specs=any_,
            scratch_shapes=[dma(())],
            compiler_params=pltpu.CompilerParams(vmem_limit_bytes=2**22),
            name="place",
        )(pieces)

    states, cache, columns, rows_of = P("dp", None), P("dp", None, "tp", None), P(None, "tp"), P("tp", None)
    return jax.shard_map(
        step,
        mesh=mesh,
        in_specs=(states, cache, cache, P(None), columns, rows_of, P(None), columns, columns, rows_of),
        out_specs=states,
        check_vma=False,
    )
```

```python
import functools

import jax
import jax.numpy as jnp
import numpy as np
from jax import lax
from jax.experimental import pallas as pl
from jax.experimental.pallas import tpu as pltpu
from jax.sharding import PartitionSpec as P

HEAD = 128
THETA = 10000
F32, BF16 = jnp.float32, jnp.bfloat16

DEEP, WIDE = 4096, 256
SLOTS = 24
LIMIT = 62 * 2**20
HELD = 8


def mult(v, k):
    return pl.multiple_of(v, k)


def layer(n, x_hbm, kc, vc, gain_a_hbm, wq, wo, gain_m_hbm, wg, wu, wd, trig_hbm, y,
          ring, x, ab, states, part, hidden, q3, seen3, gain_a, gain_m, trig, box1, box2, stage1, stage2,
          slot_sem, x_sem, send1, send2, recv1, recv2):
    me = lax.axis_index("tp")
    rows, d = x_hbm.shape
    head = kc.shape[2]
    keys = kc.shape[1]
    up_blocks = wg.shape[1] // WIDE
    down_rows = wd.shape[0]
    down_blocks = d // WIDE
    mlp = 4 * up_blocks + down_blocks
    chunk_rows = 16
    chunks = rows // chunk_rows

    def put(src, dst, slot):
        pltpu.make_async_copy(src, dst, slot_sem.at[slot]).start()

    def ready(slot, deep=DEEP):
        pltpu.make_async_copy(wg.at[pl.ds(0, deep), pl.ds(0, WIDE)], ring.at[slot, pl.ds(0, deep)], slot_sem.at[slot]).wait()

    def start_wq(cb, part_):
        slot = 2 * cb + part_
        put(wq.at[pl.ds(part_ * DEEP, DEEP), pl.ds(mult(cb * WIDE, WIDE), WIDE)], ring.at[slot], slot)

    def start_wo(cb):
        slot = HELD + cb
        for j in range(4):
            put(wo.at[:, pl.ds(mult(cb * 4 * WIDE + j * WIDE, WIDE), WIDE)], ring.at[slot, pl.ds(j * 1024, 1024)], slot)

    def kv_slot(j):
        return lax.rem(2 * HELD + lax.rem(j, SLOTS - HELD), SLOTS)

    def start_kv(it):
        for which, src in enumerate((kc, vc)):
            slot = kv_slot(2 * it + which)
            for p in range(2):
                for side in range(2):
                    put(src.at[it * 4 + 2 * p + side], ring.at[slot, pl.ds(p * keys, keys), pl.ds(side * head, head)], slot)

    def mlp_slot(m):
        return lax.rem(2 * HELD + m, SLOTS)

    def start_mlp4(m):
        @pl.when(m < 4 * up_blocks)
        def _():
            col = pl.ds(mult(m // 4 * WIDE, WIDE), WIDE)
            for r in range(4):
                slot = mlp_slot(m + r)
                put((wg, wu)[r // 2].at[pl.ds(r % 2 * DEEP, DEEP), col], ring.at[slot], slot)

        @pl.when((m >= 4 * up_blocks) & (m < mlp))
        def _():
            for r in range(4):
                slot = mlp_slot(m + r)
                nb = m + r - 4 * up_blocks
                put(wd.at[:, pl.ds(mult(nb * WIDE, WIDE), WIDE)], ring.at[slot, pl.ds(0, down_rows)], slot)

    small = [pltpu.make_async_copy(a, b, x_sem.at[i]) for i, (a, b) in enumerate(
        ((x_hbm, x), (gain_a_hbm, gain_a), (gain_m_hbm, gain_m), (trig_hbm, trig)))]
    for copy in small:
        copy.start()
    for cb in range(2):
        for part_ in range(2):
            start_wq(cb, part_)
    barrier = pltpu.get_barrier_semaphore()
    for step in (1, 2, n - 2, n - 1):
        pl.semaphore_signal(barrier, inc=1, device_id={"tp": lax.rem(me + step, n)}, device_id_type=pl.DeviceIdType.MESH)

    def steps(s, g, piece_rows, box, stage, send, recv, whole, residual, done):
        sign = 1 - 2 * lax.rem(g + lax.axis_index("dp"), 2)

        def dev(k):
            return lax.rem(me + k * sign + 2 * n, n)

        def at(o):
            return pl.ds(mult((g * n + o) * piece_rows, piece_rows), piece_rows)

        def remote(i, src, dst, to):
            return pltpu.make_async_remote_copy(src_ref=src, dst_ref=dst, send_sem=send.at[g, i], recv_sem=recv.at[g, i],
                                                device_id={"tp": dev(to)}, device_id_type=pl.DeviceIdType.MESH)

        def term(i, to):
            return remote(i, stage.at[g, i], box.at[g, i], to)

        def piece(i, owner, to):
            ref = whole.at[at(dev(owner))]
            return remote(7 + i, ref, ref, to)

        def send_term(i, owner, to, *terms):
            value = part[at(dev(owner)), :]
            for k in terms:
                term(k, 0).wait_recv()
                value = value + box[g, k].astype(F32)
            stage[g, i] = value.astype(BF16)
            term(i, to).start()

        if s == 0:
            send_term(0, 4, 2)
            send_term(1, 3, 1)
            send_term(3, -3, -1)
            send_term(2, 1, 1)
            send_term(4, -1, -1)
        if s == 1:
            send_term(6, -2, -2, 3)
            send_term(5, 2, 2, 1, 0)
        if s == 2:
            value = part[at(me), :]
            for k in (2, 4, 6, 5):
                term(k, 0).wait_recv()
                value = value + box[g, k].astype(F32)
            whole[at(me), :] = (residual(g) + value).astype(BF16)
            for i, to in ((0, 2), (2, -2), (1, 1), (3, -1)):
                piece(i, 0, to).start()
        if s == 3:
            piece(2, 2, 0).wait_recv()
            piece(6, 2, -1).start()
            piece(0, -2, 0).wait_recv()
            piece(4, -2, 2).start()
            piece(5, -2, 1).start()
        if s == 4:
            for i, owner in ((1, -1), (3, 1), (4, -4), (5, -3), (6, 3)):
                piece(i, owner, 0).wait_recv()
            done(g)
        if s == 5:
            for i in range(7):
                term(i, 1).wait_send()
                piece(i, 0, 1).wait_send()

    LAST = 4

    blocks = d // 128

    def norm_x(i, _):
        r = pl.ds(mult(i * 16, 16), 16)
        total = jnp.zeros((16, 128), F32)
        for k in range(blocks):
            wide = x[r, pl.ds(k * 128, 128)].astype(F32)
            total = total + wide * wide
        scale = lax.rsqrt(jnp.sum(total, -1, keepdims=True) * (1.0 / d) + 1e-6)
        for k in range(blocks):
            c = pl.ds(k * 128, 128)
            ab[r, c] = (x[r, c].astype(F32) * scale * gain_a[k:k + 1, :].astype(F32)).astype(BF16)
        return 0

    for copy in small:
        copy.wait()
    for cb in (2, 3):
        for part_ in range(2):
            start_wq(cb, part_)
    start_kv(0)
    with jax.named_scope("norm"):
        lax.fori_loop(0, rows // 16, norm_x, 0)
    for it in range(1, 4):
        start_kv(it)

    def project(cb, _):
        ready(2 * cb)
        ready(2 * cb + 1)
        acc = jnp.dot(ab[:, pl.ds(0, DEEP)], ring[2 * cb], preferred_element_type=F32)
        acc = acc + jnp.dot(ab[:, pl.ds(DEEP, DEEP)], ring[2 * cb + 1], preferred_element_type=F32)
        for j in range(2):
            t = acc[:, j * head:(j + 1) * head].astype(BF16).astype(F32)
            t = t * trig[0:1, :] + pltpu.roll(t, head // 2, 1) * trig[1:2, :]
            q3[pl.ds(2 * cb + j, rows, stride=8), :] = t.astype(BF16).astype(F32)
        start_kv(4 + cb)
        start_wo(2 * cb)
        start_wo(2 * cb + 1)
        return 0

    with jax.named_scope("project"):
        lax.fori_loop(0, 4, project, 0)
    pl.semaphore_wait(barrier, 4)

    def residual1(g):
        r = pl.ds(mult(g * chunk_rows, chunk_rows), chunk_rows)
        cols = [x[r, pl.ds(mult(me * 1024 + k * 128, 128), 128)].astype(F32) for k in range(8)]
        return jnp.concatenate(cols, 0)

    def done1(g):
        total = jnp.zeros((chunk_rows, 128), F32)
        for k in range(blocks):
            wide = states[pl.ds(mult(g * 1024 + k * 16, 16), 16), :].astype(F32)
            total = total + wide * wide
        scale = lax.rsqrt(jnp.sum(total, -1, keepdims=True) * (1.0 / d) + 1e-6)
        r = pl.ds(mult(g * chunk_rows, chunk_rows), chunk_rows)
        for k in range(blocks):
            c = pl.ds(k * 128, 128)
            wide = states[pl.ds(mult(g * 1024 + k * 16, 16), 16), :].astype(F32)
            ab[r, c] = (wide * scale * gain_m[k:k + 1, :].astype(F32)).astype(BF16)

    first = functools.partial(steps, piece_rows=chunk_rows * 8, box=box1, stage=stage1, send=send1, recv=recv1,
                              whole=states, residual=residual1, done=done1)

    def attend(it):
        ks, vs = kv_slot(2 * it), kv_slot(2 * it + 1)
        ready(ks)
        ready(vs)
        zero = jnp.zeros((8, head), F32)
        weights = []
        for p in range(2):
            s0 = (it * 4 + 2 * p) * 8
            q = jnp.concatenate([jnp.concatenate([q3[pl.ds(mult(s0, 8), 8), :], zero], 1),
                                 jnp.concatenate([zero, q3[pl.ds(mult(s0 + 8, 8), 8), :]], 1)], 0).astype(BF16)
            scores = lax.dot_general(q, ring[ks, pl.ds(p * keys, keys)], (((1,), (1,)), ((), ())),
                                     preferred_element_type=F32) * head**-0.5
            e = jnp.exp(scores - jnp.max(scores, -1, keepdims=True))
            weights.append((e * (1.0 / jnp.sum(e, -1, keepdims=True))).astype(BF16))
        for p in range(2):
            s0 = (it * 4 + 2 * p) * 8
            o = jnp.dot(weights[p], ring[vs, pl.ds(p * keys, keys)], preferred_element_type=F32)
            o = o.astype(BF16).astype(F32)
            seen3[pl.ds(mult(s0, 8), 8), :] = o[:8, :head]
            seen3[pl.ds(mult(s0 + 8, 8), 8), :] = o[8:, head:]

        @pl.when(it < 8)
        def _():
            start_kv(it + 8)

    def wo_pass(row0, count):
        seen = jnp.concatenate([seen3[pl.ds(row0 * 8 + h, count, stride=8), :] for h in range(8)], 1).astype(BF16)

        def columns(cb2, _):
            for k in range(2):
                @pl.when(row0 == 0)
                def _():
                    ready(HELD + 2 * cb2 + k)

            for k in range(2):
                cb = 2 * cb2 + k
                for j in range(4):
                    acc = jnp.dot(seen, ring[HELD + cb, pl.ds(j * 1024, 1024)], preferred_element_type=F32)
                    for r in range(count // 16):
                        base = ((row0 // 16 + r) * 8 + cb) * 128 + j * 32
                        part[pl.ds(mult(base, 16), 16), :] = acc[r * 16:(r + 1) * 16, :128]
                        part[pl.ds(mult(base + 16, 16), 16), :] = acc[r * 16:(r + 1) * 16, 128:]
            return 0

        with jax.named_scope("wo"):
            lax.fori_loop(0, 4, columns, 0)

    def sequences(it, _):
        with jax.named_scope("attend"):
            attend(it)

        @pl.when((lax.rem(it, 2) == 1) & (it >= 8))
        def _():
            start_mlp4(2 * (it - 1 - 8))

        @pl.when(it == 9)
        def _():
            wo_pass(0, 32)
            lax.fori_loop(0, 2, run1(0), 0)

        @pl.when(it == 13)
        def _():
            lax.fori_loop(0, 2, run1(1), 0)

        @pl.when((it == 12) | (it == 15))
        def _():
            c = (it - 6) // 3
            wo_pass(c * 16, 16)
            run1(0)(c, 0)
        return 0

    def run1(s):
        def body(g, _):
            with jax.named_scope(f"a{s}"):
                first(s, g)
            return 0
        return body

    lax.fori_loop(0, 16, sequences, 0)
    start_mlp4(16)
    start_mlp4(20)

    for s, lo, hi in ((1, 2, 3), (2, 0, 2), (1, 3, 4), (2, 2, 3), (3, 0, 2), (2, 3, 4), (3, 2, 3), (4, 0, 2), (3, 3, 4), (4, 2, 4)):
        lax.fori_loop(lo, hi, run1(s), 0)

    def gate_up(cb, _):
        m = 4 * cb
        outs = []
        for r in range(4):
            ready(mlp_slot(m + r))
        for r in range(2):
            s0, s1 = mlp_slot(m + 2 * r), mlp_slot(m + 2 * r + 1)
            acc = jnp.dot(ab[:, pl.ds(0, DEEP)], ring[s0], preferred_element_type=F32)
            outs.append(acc + jnp.dot(ab[:, pl.ds(DEEP, DEEP)], ring[s1], preferred_element_type=F32))
        hidden[:, pl.ds(mult(cb * WIDE, WIDE), WIDE)] = (jax.nn.silu(outs[0]) * outs[1]).astype(BF16)
        start_mlp4(m + SLOTS)
        return 0

    with jax.named_scope("gate_up"):
        lax.fori_loop(0, up_blocks, gate_up, 0)

    def residual2(g):
        pieces = [states[pl.ds(mult(c * 1024 + g * 128 + me * 16, 16), 16), :] for c in range(chunks)]
        return jnp.concatenate(pieces, 0).astype(F32)

    groups = d // 1024

    second = functools.partial(steps, piece_rows=rows, box=box2, stage=stage2, send=send2, recv=recv2,
                               whole=y, residual=residual2, done=lambda g: None)

    def run2(s):
        def body(g, _):
            with jax.named_scope(f"b{s}"):
                second(s, g)
            return 0
        return body

    def down(t, _):
        with jax.named_scope("down"):
            for i in range(4):
                ready(mlp_slot(4 * up_blocks + 4 * t + i), down_rows)
            for i in range(4):
                nb = 4 * t + i
                slot = mlp_slot(4 * up_blocks + nb)
                acc = jnp.dot(hidden[...], ring[slot, pl.ds(0, down_rows)], preferred_element_type=F32)
                part[pl.ds(mult(nb * 2 * rows, rows), rows), :] = acc[:, :128]
                part[pl.ds(mult(nb * 2 * rows + rows, rows), rows), :] = acc[:, 128:]
        start_mlp4(4 * up_blocks + 4 * t + SLOTS)
        for s, lag in enumerate(LAGS):
            @pl.when(t >= lag)
            def _():
                run2(s)(t - lag, 0)
        return 0

    LAGS = (0, 2, 4, 7)
    lax.fori_loop(0, groups, down, 0)
    for s, g in ((1, 6), (3, 1), (2, 4), (1, 7), (3, 2), (2, 5), (3, 3), (2, 6), (3, 4), (2, 7), (3, 5), (3, 6), (3, 7)):
        run2(s)(jnp.int32(g), 0)
    lax.fori_loop(0, chunks, run1(LAST + 1), 0)
    lax.fori_loop(0, groups - 2, run2(LAST + 1), 0)
    lax.fori_loop(0, groups, run2(LAST), 0)
    lax.fori_loop(groups - 2, groups, run2(LAST + 1), 0)


def place(y, out, sem):
    rows, d = out.shape

    def copy(p):
        return pltpu.make_async_copy(y.at[pl.ds(mult(p * rows, rows), rows)], out.at[:, pl.ds(mult(p * 128, 128), 128)], sem)

    lax.fori_loop(0, d // 128, lambda p, _: (copy(p).start(), 0)[1], 0)
    pltpu.make_async_copy(y, y, sem).wait()


def solution(mesh):
    n = mesh.shape["tp"]

    def step(x, k_cache, v_cache, gain_a, wq, wo, gain_m, w_gate, w_up, w_down):
        rows, d = x.shape
        batch, keys, _, head = k_cache.shape
        ff = w_gate.shape[1]
        half = head // 2
        angle = np.float32(keys - 1) * THETA ** (-np.arange(half) / half)
        cos, sin = np.cos(angle), np.sin(angle)
        trig = jnp.asarray(np.stack([np.concatenate([cos, cos]), np.concatenate([-sin, sin])]), F32)
        any_ = pl.BlockSpec(memory_space=pl.ANY)
        chunks, groups = rows // 16, d // 1024
        dma = pltpu.SemaphoreType.DMA
        pieces = pl.pallas_call(
            functools.partial(layer, n),
            out_shape=pltpu.VMEM((rows * d // 128, 128), BF16),
            in_specs=[any_] * 11,
            out_specs=pl.BlockSpec(memory_space=pltpu.VMEM),
            scratch_shapes=[
                pltpu.VMEM((SLOTS, DEEP, WIDE), BF16),
                pltpu.VMEM((rows, d), BF16),
                pltpu.VMEM((rows, d), BF16),
                pltpu.VMEM((rows * d // 128, 128), BF16),
                pltpu.VMEM((rows * d // 128, 128), F32),
                pltpu.VMEM((rows, ff), BF16),
                pltpu.VMEM((rows * 8, head), F32),
                pltpu.VMEM((rows * 8, head), F32),
                pltpu.VMEM((d // 128, 128), BF16),
                pltpu.VMEM((d // 128, 128), BF16),
                pltpu.VMEM((2, 128), F32),
                pltpu.VMEM((chunks, 7, 128, 128), BF16),
                pltpu.VMEM((groups, 7, rows, 128), BF16),
                pltpu.VMEM((chunks, 7, 128, 128), BF16),
                pltpu.VMEM((groups, 7, rows, 128), BF16),
                dma((SLOTS,)),
                dma((4,)),
                dma((chunks, 14)),
                dma((groups, 14)),
                dma((chunks, 14)),
                dma((groups, 14)),
            ],
            compiler_params=pltpu.CompilerParams(collective_id=0, has_side_effects=True, vmem_limit_bytes=LIMIT),
            name="decoder_layer",
        )(x, k_cache.reshape(batch, keys, head), v_cache.reshape(batch, keys, head), gain_a.reshape(d // 128, 128), wq, wo,
          gain_m.reshape(d // 128, 128), w_gate, w_up, w_down, trig)
        return pl.pallas_call(
            place,
            out_shape=jax.ShapeDtypeStruct((rows, d), BF16),
            in_specs=[pl.BlockSpec(memory_space=pltpu.VMEM)],
            out_specs=any_,
            scratch_shapes=[dma(())],
            compiler_params=pltpu.CompilerParams(vmem_limit_bytes=2**22),
            name="place",
        )(pieces)

    states, cache, columns, rows_of = P("dp", None), P("dp", None, "tp", None), P(None, "tp"), P("tp", None)
    return jax.shard_map(
        step,
        mesh=mesh,
        in_specs=(states, cache, cache, P(None), columns, rows_of, P(None), columns, columns, rows_of),
        out_specs=states,
        check_vma=False,
    )
```
